256 devices in a mesh: band: 64 (over y, z, core), mp: 4 (over x).
Axes of the slice: x: 4, y: 4, z: 8, core: 2. Of those that a mesh axis runs over, the one named last changes fastest.
Arguments:
- grid_latent: bfloat16 [262144, 512], P('band'), may hold values from -6 to 6
- edge_latent: bfloat16 [393216, 512], P('band'), may hold values from -6 to 6
- mesh_latent: bfloat16 [40960, 512], P('band', 'mp'), may hold values from -6 to 6
- mesh_grad: bfloat16 [40960, 512], P('band', 'mp'), may hold values from -96 to 96
- counts: int32 [40960], P('band'), may hold values from 8 to 64
- request: int32 [64, 7, 128], P('band'), may hold values from -1 to 639, as said below
- edge_sender: int32 [393216], P('band'), may hold values from 0 to 4095, as said below
- edge_slot: int32 [393216], P('band'), may hold values from 0 to 895, as said below
- w_send: bfloat16 [512, 512], P(None, 'mp'), may hold values from -0.25 to 0.25
- w_recv: bfloat16 [512, 512], P(None, 'mp'), may hold values from -0.25 to 0.25
- w_edge: bfloat16 [512, 512], P(None, 'mp'), may hold values from -0.25 to 0.25
- edge_bias: float32 [512], P('mp'), may hold values from -3 to 3
- w_out: bfloat16 [512, 512], P('mp'), may hold values from -0.25 to 0.25
Outputs:
- grid_grad: bfloat16 [262144, 512], P('band', 'mp')
- node_grad: bfloat16 [40960, 512], P('band', 'mp')
The draws below stay inside these ranges and needn't reach their ends.
Inputs may be any that keep to these rules, and one draw needn't show every extreme that they name: request[p, k, c] is a node of patch p, numbered within the patch, wanted by band p + 3 - k, or -1 for an empty slot; where that band lies outside 0 to 63 all slots are -1; otherwise the live slots come first, name distinct nodes and number 1 or more; request[p, 3, c] is live for every c. `edge_sender`: within a band the senders never fall, and each grid point of the band sends one or two edges. edge_slot = k * 128 + c, the patch b + k - 3 of the edge's band b lies in 0 to 63, and request[b + k - 3, k, c] is never -1.
All inputs are finite; a program needn't handle non-finite values.
Results may differ from the reference program's by a relative error of at most 0.015.
Values may be sent and summed in bfloat16 or wider, within the bound.
No kernel may reach another device: no remote copies, remote signals or barrier semaphores. Data moves between devices by JAX's collectives and lax.ppermute only.
A program may use at most 64 MiB of HBM per device.

```python
import jax
import jax.numpy as jnp
from jax import lax

LATENT = 512
HIDDEN_SIZE = 512
G_DEV = 4096
EDGE_DEV = 6144
M_DEV = 640
CAPACITY = 128
REACH = 3
SPAN = 7
GRID = 262144
EDGES = 393216
MESH = 40960
N_BAND = 64


def live_counts(key):
    band_index = jnp.arange(N_BAND, dtype=jnp.int32)
    offsets = jnp.arange(SPAN, dtype=jnp.int32)
    patches = band_index[:, None] + offsets[None, :] - REACH
    inside = (patches >= 0) & (patches < N_BAND)
    distance = jnp.abs(offsets - REACH)
    highest = CAPACITY - distance * CAPACITY // (REACH + 1)
    jitter = jax.random.randint(key, (N_BAND, SPAN), 0, CAPACITY // 8 + 1)
    lowered = jnp.clip(highest[None, :] - jitter, 1, CAPACITY)
    lowered = jnp.where((distance == 0)[None, :], CAPACITY, lowered)
    return jnp.where(inside, lowered, 0).astype(jnp.int32)


def draw_request(key, part):
    live = live_counts(jax.random.fold_in(key, 7))
    patch_index = jnp.arange(N_BAND, dtype=jnp.int32)
    offsets = jnp.arange(SPAN, dtype=jnp.int32)
    bands = patch_index[:, None] + REACH - offsets[None, :]
    inside = (bands >= 0) & (bands < N_BAND)
    band_clip = jnp.clip(bands, 0, N_BAND - 1)
    live_here = jnp.where(inside, live[band_clip, offsets[None, :]], 0)
    scores = jax.random.randint(jax.random.fold_in(key, 11), (N_BAND, SPAN, M_DEV), 0, 1 << 20)
    scores = scores * M_DEV + jnp.arange(M_DEV, dtype=jnp.int32)
    ordered = jnp.argsort(scores, axis=-1)[:, :, :CAPACITY].astype(jnp.int32)
    column = jnp.arange(CAPACITY, dtype=jnp.int32)
    return jnp.where(column[None, None, :] < live_here[:, :, None], ordered, -1).astype(jnp.int32)


def draw_edge_slot(key, part):
    live = live_counts(jax.random.fold_in(key, 7))
    first_key, second_key = jax.random.split(jax.random.fold_in(key, 13))
    band_index = jnp.arange(N_BAND, dtype=jnp.int32)
    lowest = jnp.maximum(0, REACH - band_index)
    highest = jnp.minimum(SPAN - 1, REACH + N_BAND - 1 - band_index) + 1
    offset = lowest[:, None] + jax.random.randint(first_key, (N_BAND, EDGE_DEV), 0, (highest - lowest)[:, None])
    bounds = jnp.take_along_axis(live, offset, axis=1)
    column = jax.random.randint(second_key, (N_BAND, EDGE_DEV), 0, bounds)
    return (offset * CAPACITY + column).reshape(-1).astype(jnp.int32)


def draw_edge_sender(key, part):
    scores = jax.random.randint(key, (N_BAND, G_DEV), 0, 1 << 18) * G_DEV + jnp.arange(G_DEV, dtype=jnp.int32)
    ranking = jnp.argsort(jnp.argsort(scores, axis=-1), axis=-1)
    repeats = 1 + (ranking < G_DEV // 2).astype(jnp.int32)

    def spread(repeat_row):
        return jnp.repeat(jnp.arange(G_DEV, dtype=jnp.int32), repeat_row, total_repeat_length=EDGE_DEV)
    return jax.vmap(spread)(repeats).reshape(-1).astype(jnp.int32)


def place_ends(entries, stream_key, low, high):
    index_at = [jax.random.randint(jax.random.fold_in(stream_key, axis), (), 0, length) for axis, length in enumerate(entries.shape)]
    widest = entries.shape.index(max(entries.shape))
    neighbour = index_at[:widest] + [(index_at[widest] + 1) % entries.shape[widest]] + index_at[widest + 1:]
    return entries.at[tuple(index_at)].set(low).at[tuple(neighbour)].set(high)


def levels(own_key, extent, shards, low, top_value):
    factor_of = 1.0
    for position, shards_of in shards:
        steps = jax.random.uniform(jax.random.fold_in(jax.random.fold_in(own_key, 6), position), (shards_of,), jnp.float32, low / len(shards), top_value / len(shards))
        factor_of = factor_of * jnp.repeat(jnp.exp(steps), extent[position] // shards_of).reshape((-1,) + (1,) * (len(extent) - 1 - position))
    return factor_of


def normal_values(key, extent, scale, bound, cuts=(), kind=jnp.bfloat16):
    result = jax.random.normal(key, extent, jnp.float32) * scale
    if len(cuts) > 0:
        result = levels(key, extent, cuts, -0.22, 0.18) * result
    return jnp.clip(result, min=-bound, max=bound).astype(kind)


def setup_inputs(seed: int = 0) -> dict:
    splits = jax.random.split(jax.random.key(seed), 14)
    grid_latent = normal_values(splits[0], (GRID, LATENT), 1.0, 6.0, ((0, 64),))
    edge_latent = normal_values(splits[1], (EDGES, LATENT), 1.0, 6.0, ((0, 64),))
    mesh_latent = normal_values(splits[2], (MESH, LATENT), 1.0, 6.0, ((0, 64), (1, 4)))
    mesh_grad = normal_values(splits[3], (MESH, LATENT), 16.0, 96.0, ((0, 64), (1, 4)))
    counts = place_ends(jax.random.randint(splits[4], (MESH,), 8, 65), jax.random.fold_in(splits[4], 1), 8, 64).astype(jnp.int32)
    request = draw_request(jax.random.fold_in(splits[13], 71), 0)
    edge_sender = draw_edge_sender(jax.random.fold_in(splits[13], 71), 0)
    edge_slot = draw_edge_slot(jax.random.fold_in(splits[13], 71), 0)
    w_send = normal_values(splits[8], (LATENT, HIDDEN_SIZE), LATENT ** -0.5, 0.25, ((1, 4),))
    w_recv = normal_values(splits[9], (LATENT, HIDDEN_SIZE), LATENT ** -0.5, 0.25, ((1, 4),))
    w_edge = normal_values(splits[10], (LATENT, HIDDEN_SIZE), LATENT ** -0.5, 0.25, ((1, 4),))
    edge_bias = normal_values(splits[11], (HIDDEN_SIZE,), 0.5, 3.0, ((0, 4),), jnp.float32)
    w_out = normal_values(splits[12], (HIDDEN_SIZE, LATENT), HIDDEN_SIZE ** -0.5, 0.25, ((0, 4),))
    return {"grid_latent": grid_latent, "edge_latent": edge_latent, "mesh_latent": mesh_latent, "mesh_grad": mesh_grad, "counts": counts, "request": request, "edge_sender": edge_sender, "edge_slot": edge_slot, "w_send": w_send, "w_recv": w_recv, "w_edge": w_edge, "edge_bias": edge_bias, "w_out": w_out}


def silu_slope(pre_act):
    sigmoid_value = jax.nn.sigmoid(pre_act)
    return sigmoid_value * (1.0 + pre_act * (1.0 - sigmoid_value))


def reference(grid_latent, edge_latent, mesh_latent, mesh_grad, counts, request, edge_sender, edge_slot, w_send, w_recv, w_edge, edge_bias, w_out):
    scaled_grad = (mesh_grad.astype(jnp.float32) / counts.astype(jnp.float32)[:, None]).astype(jnp.bfloat16)
    node_proj = jnp.dot(mesh_latent, w_recv, preferred_element_type=jnp.float32)
    node_back = jnp.dot(scaled_grad, w_out.T, preferred_element_type=jnp.float32)
    recv_wide = w_recv.astype(jnp.float32)
    offsets = jnp.arange(SPAN, dtype=jnp.int32)

    def per_band(node_sum, band_index):
        grid_rows = lax.dynamic_slice_in_dim(grid_latent, band_index * G_DEV, G_DEV, 0)
        edge_rows = lax.dynamic_slice_in_dim(edge_latent, band_index * EDGE_DEV, EDGE_DEV, 0)
        senders = lax.dynamic_slice_in_dim(edge_sender, band_index * EDGE_DEV, EDGE_DEV, 0)
        slot_ids = lax.dynamic_slice_in_dim(edge_slot, band_index * EDGE_DEV, EDGE_DEV, 0)
        patches = (band_index + offsets - REACH).astype(jnp.int32)
        inside = (patches >= 0) & (patches < N_BAND)
        patch_clip = jnp.clip(patches, 0, N_BAND - 1).astype(jnp.int32)
        slot_table = request[patch_clip, offsets]
        slot_table = jnp.where(inside[:, None], slot_table, -1).reshape(-1)
        local_node = slot_table[slot_ids]
        patch_of = patch_clip[slot_ids // CAPACITY]
        is_live = (local_node >= 0)[:, None]
        receiver = (patch_of * M_DEV + jnp.maximum(local_node, 0)).astype(jnp.int32)
        grid_proj = jnp.dot(grid_rows, w_send, preferred_element_type=jnp.float32)
        pre_act = grid_proj[senders] + jnp.where(is_live, node_proj[receiver], 0.0)
        pre_act = pre_act + jnp.dot(edge_rows, w_edge, preferred_element_type=jnp.float32) + edge_bias.astype(jnp.float32)
        edge_grad = (jnp.where(is_live, node_back[receiver], 0.0) * silu_slope(pre_act)).astype(jnp.bfloat16)
        wide_grad = edge_grad.astype(jnp.float32)
        sender_sum = jax.ops.segment_sum(wide_grad, senders, num_segments=G_DEV).astype(jnp.bfloat16)
        grid_block = jnp.dot(sender_sum, w_send.T, preferred_element_type=jnp.float32).astype(jnp.bfloat16)
        node_sum = node_sum.at[receiver].add(jnp.where(is_live, wide_grad, 0.0))
        return node_sum, grid_block

    initial = jnp.zeros((M_DEV * N_BAND, HIDDEN_SIZE), jnp.float32)
    node_sum, grid_blocks = lax.scan(per_band, initial, jnp.arange(N_BAND, dtype=jnp.int32))
    grid_grad = grid_blocks.reshape(G_DEV * N_BAND, LATENT)
    node_grad = jnp.dot(node_sum, recv_wide.T, precision=lax.Precision.HIGHEST).astype(jnp.bfloat16)
    return grid_grad, node_grad
```

```python
import jax
import jax.numpy as jnp
from jax import lax
from jax.experimental import pallas as pl
from jax.experimental.pallas import tpu as pltpu
from jax.sharding import PartitionSpec as P


F32 = jnp.float32
BF16 = jnp.bfloat16
I32 = jnp.int32
LANES = 128
BLOCK = 256
WINDOW = 384
NEAR = (3, 2, 4)
FAR = (1, 5, 0, 6)


def ring(shard, axis, by):
    devices = lax.axis_size(axis)
    return lax.ppermute(shard, axis, [(i, (i + by) % devices) for i in range(devices)])


def from_peers(shard, by_shift):
    return [ring(shard[s] if by_shift else shard, "mp", s) for s in (1, 2, 3)]


def dot(a, b):
    return jnp.dot(a, b, preferred_element_type=F32)


def dot_t(a, b):
    return lax.dot_general(a, b, (((1,), (1,)), ((), ())), preferred_element_type=F32)


def column(row):
    return jnp.transpose(jnp.broadcast_to(row, (LANES, row.shape[1])))


def one_hot(ids, width):
    lane = lax.broadcasted_iota(I32, ids.shape, 1)
    parts = [(ids == lane + LANES * t).astype(F32).astype(BF16) for t in range(width // LANES)]
    return jnp.concatenate(parts, axis=1)


def one_hot_t(row, height):
    shape = (height, row.shape[1])
    return (jnp.broadcast_to(row, shape) == lax.broadcasted_iota(I32, shape, 0)).astype(F32).astype(BF16)


def call(kernel, out_shape, args, flops, nbytes, **kw):
    return pl.pallas_call(
        kernel,
        out_shape=out_shape,
        cost_estimate=pl.CostEstimate(flops=flops, bytes_accessed=nbytes, transcendentals=0),
        **kw,
    )(*args)


def shape(dims, dtype):
    return jax.ShapeDtypeStruct(dims, dtype)


def full_spec(dims):
    zeros = (0,) * len(dims)
    return pl.BlockSpec(dims, lambda *_: zeros)


def pick_kernel(lat_ref, grad_ref, counts_ref, req_ref, *out_refs):
    nodes = lat_ref.shape[0]
    scaled = []
    for t in range(nodes // LANES):
        rows = pl.ds(LANES * t, LANES)
        count = column(counts_ref[t : t + 1, :]).astype(F32)
        scaled.append((grad_ref[rows, :].astype(F32) / count).astype(BF16))
    both = jnp.concatenate([lat_ref[...], jnp.concatenate(scaled, axis=0)], axis=1)
    for k, out_ref in enumerate(out_refs):
        ids = column(req_ref[k : k + 1, :])
        out_ref[...] = dot(one_hot(ids, nodes), both).astype(BF16)


def grid_kernel(x_ref, w_ref, out_ref):
    proj = dot(x_ref[...], w_ref[...])
    upper = proj.astype(BF16)
    lower = (proj - upper.astype(F32)).astype(BF16)
    out_ref[...] = jnp.concatenate([upper, lower], axis=1)


def pre_kernel(base_ref, edge_ref, send_ref, split_ref, w_ref, bias_ref, out_ref):
    cols = w_ref.shape[1]
    step = pl.program_id(0)
    per_step = edge_ref.shape[0] // BLOCK
    for sub in range(per_step):
        block = step * per_step + sub
        rows = pl.ds(sub * BLOCK, BLOCK)
        base = pl.multiple_of(base_ref[block], LANES)
        ids = column(send_ref[pl.ds(block, 1), :]) - base
        picked = dot(one_hot(ids, WINDOW), split_ref[pl.ds(base, WINDOW), :])
        value = picked[:, :cols] + picked[:, cols:] + dot(edge_ref[rows, :], w_ref[...])
        out_ref[rows, :] = value + bias_ref[...]


def main_kernel(base_ref, chan_ref, *refs):
    near, far = refs[:4], refs[4:8]
    recv_ref, wout_ref, pre_ref, send_ref, slot_ref = refs[8:13]
    sums, slots = refs[13:17], refs[17:24]
    table_ref, acc_ref, slot_acc_ref = refs[24:]
    cols = recv_ref.shape[1]
    step = pl.program_id(0)
    per_step = pre_ref.shape[0] // BLOCK

    @pl.when(step == 0)
    def _():
        acc_ref[...] = jnp.zeros_like(acc_ref)
        slot_acc_ref[...] = jnp.zeros_like(slot_acc_ref)
        for group, ks in ((near, NEAR), (far, FAR)):
            proj = back = None
            for s, ref in enumerate(group):
                chan = pl.ds(pl.multiple_of(chan_ref[s], LANES), LANES)
                p = dot(ref[:, :LANES], recv_ref[chan, :])
                b = dot_t(ref[:, LANES:], wout_ref[:, chan])
                proj = p if proj is None else proj + p
                back = b if back is None else back + b
            both = jnp.concatenate([proj, back], axis=1).astype(BF16)
            for n, k in enumerate(ks):
                table_ref[k * LANES : (k + 1) * LANES, :] = both[n * LANES : (n + 1) * LANES, :]

    slot_count = table_ref.shape[0]
    for sub in range(per_step):
        block = step * per_step + sub
        rows = pl.ds(sub * BLOCK, BLOCK)
        slot_row = slot_ref[pl.ds(block, 1), :]
        got = dot(one_hot(column(slot_row), slot_count), table_ref[...])
        pre = pre_ref[rows, :] + got[:, :cols]
        sig = jax.nn.sigmoid(pre)
        grad = (got[:, cols:] * (sig * (1.0 + pre * (1.0 - sig)))).astype(BF16)
        slot_acc_ref[...] += dot(one_hot_t(slot_row, slot_count), grad)
        base = pl.multiple_of(base_ref[block], LANES)
        send_row = send_ref[pl.ds(block, 1), :] - base
        acc_ref[pl.ds(base, WINDOW), :] += dot(one_hot_t(send_row, WINDOW), grad)

    @pl.when(step == pl.num_programs(0) - 1)
    def _():
        quarter = sums[0].shape[0]
        for s, out_ref in enumerate(sums):
            first = pl.multiple_of(chan_ref[4 + s] // LANES * quarter, LANES)
            out_ref[...] = acc_ref[pl.ds(first, quarter), :].astype(BF16)
        for k, out_ref in enumerate(slots):
            out_ref[...] = slot_acc_ref[k * LANES : (k + 1) * LANES, :].astype(BF16)


def back_kernel(chan_ref, *refs):
    parts, weights, outs = refs[:4], refs[4:8], refs[8:12]
    x = jnp.concatenate([r[...] for r in parts], axis=1)
    for s, out_ref in enumerate(outs):
        chan = pl.ds(pl.multiple_of(chan_ref[4 + s], LANES), LANES)
        w = jnp.concatenate([r[chan, :] for r in weights], axis=1)
        out_ref[...] = dot_t(x, w).astype(BF16)


def place_kernel(chan_ref, *refs):
    out_ref = refs[4]
    quarter = refs[0].shape[0]
    for s in range(4):
        first = pl.multiple_of(chan_ref[s] // LANES * quarter, LANES)
        out_ref[pl.ds(first, quarter), :] = refs[s][...]


def node_kernel(chan_ref, req_ref, recv_ref, *refs):
    returned, outs = refs[:7], refs[7:11]
    nodes = outs[0].shape[0]
    total = None
    for k, ref in enumerate(returned):
        part = dot(one_hot_t(req_ref[k : k + 1, :], nodes), ref[...])
        total = part if total is None else total + part
    upper = total.astype(BF16)
    lower = (total - upper.astype(F32)).astype(BF16)
    for s, out_ref in enumerate(outs):
        w = recv_ref[pl.ds(pl.multiple_of(chan_ref[4 + s], LANES), LANES), :]
        out_ref[...] = (dot_t(upper, w) + dot_t(lower, w)).astype(out_ref.dtype)


def per_device(
    grid_latent,
    edge_latent,
    mesh_latent,
    mesh_grad,
    counts,
    request,
    edge_sender,
    edge_slot,
    w_send,
    w_recv,
    w_edge,
    edge_bias,
    w_out,
):
    span, capacity = request.shape[1:]
    nodes = mesh_latent.shape[0]
    grid_rows, latent = grid_latent.shape
    edges = edge_latent.shape[0]
    cols = w_send.shape[1]
    slot_count = span * capacity
    blocks = edges // BLOCK
    quarter = grid_rows // 4
    mine = lax.axis_index("mp")
    turns = jnp.arange(4, dtype=I32)
    chan = jnp.concatenate([(mine - turns) % 4, (mine + turns) % 4]).astype(I32) * LANES
    senders = edge_sender.reshape(blocks, BLOCK)
    slot_ids = edge_slot.reshape(blocks, BLOCK)
    base = jnp.minimum(senders[:, 0] // LANES * LANES, grid_rows - WINDOW)
    wanted = request[0]

    send_peers = from_peers(w_send, False)
    picked = call(
        pick_kernel,
        [shape((capacity, 2 * LANES), BF16)] * span,
        (mesh_latent, mesh_grad, counts.reshape(nodes // LANES, LANES), wanted),
        2 * slot_count * nodes * 2 * LANES,
        2 * (2 * nodes + 2 * slot_count) * LANES,
    )
    arrived = {3: picked[3]}
    for k in (2, 4, 1, 5, 0, 6):
        arrived[k] = ring(picked[k], "band", 3 - k)
    near = jnp.concatenate([arrived[k] for k in NEAR], axis=0)
    far = jnp.concatenate([arrived[k] for k in FAR], axis=0)
    near_all = [near] + from_peers(near, False)
    far_all = [far] + from_peers(far, False)

    rows = 512
    split = call(
        grid_kernel,
        shape((grid_rows, 2 * cols), BF16),
        (grid_latent, w_send),
        2 * grid_rows * latent * cols,
        2 * grid_rows * (latent + 2 * cols),
        grid=(grid_rows // rows,),
        in_specs=[pl.BlockSpec((rows, latent), lambda i: (i, 0)), full_spec(w_send.shape)],
        out_specs=pl.BlockSpec((rows, 2 * cols), lambda i: (i, 0)),
    )
    bias = edge_bias.reshape(1, cols)
    pre = call(
        pre_kernel,
        shape((edges, cols), F32),
        (base, edge_latent, senders, split, w_edge, bias),
        2 * edges * cols * (latent + 2 * WINDOW),
        2 * edges * (latent + 2 * cols) + 4 * grid_rows * cols,
        grid_spec=pltpu.PrefetchScalarGridSpec(
            num_scalar_prefetch=1,
            grid=(edges // rows,),
            in_specs=[
                pl.BlockSpec((rows, latent), lambda i, *_: (i, 0)),
                full_spec(senders.shape),
                full_spec(split.shape),
                full_spec(w_edge.shape),
                full_spec(bias.shape),
            ],
            out_specs=pl.BlockSpec((rows, cols), lambda i, *_: (i, 0)),
        ),
    )
    operands = (*near_all, *far_all, w_recv, w_out)
    out_shape = [shape((quarter, cols), BF16)] * 4 + [shape((capacity, cols), BF16)] * span
    result = call(
        main_kernel,
        out_shape,
        (base, chan, *operands, pre, senders, slot_ids),
        2 * edges * cols * (3 * slot_count + WINDOW),
        4 * edges * cols,
        grid_spec=pltpu.PrefetchScalarGridSpec(
            num_scalar_prefetch=2,
            grid=(edges // rows,),
            in_specs=[full_spec(a.shape) for a in operands]
            + [
                pl.BlockSpec((rows, cols), lambda i, *_: (i, 0)),
                full_spec(senders.shape),
                full_spec(slot_ids.shape),
            ],
            out_specs=[full_spec(s.shape) for s in out_shape],
            scratch_shapes=[
                pltpu.VMEM((slot_count, 2 * cols), BF16),
                pltpu.VMEM((grid_rows, cols), F32),
                pltpu.VMEM((slot_count, cols), F32),
            ],
        ),
    )
    sums, slot_sums = result[:4], result[4:]

    smem = pl.BlockSpec(memory_space=pltpu.SMEM)
    vmem = pl.BlockSpec(memory_space=pltpu.VMEM)
    returned = [
        slot_sums[k] if k == 3 else ring(slot_sums[k], "band", k - 3) for k in (2, 4, 1, 5, 0, 6, 3)
    ]
    order = (2, 4, 1, 5, 0, 6, 3)
    returned = [returned[order.index(k)] for k in range(span)]
    hidden_parts = [sums[0]] + from_peers(sums, True)
    terms = call(
        back_kernel,
        [shape((quarter, LANES), BF16)] * 4,
        (chan, *hidden_parts, w_send, *send_peers),
        2 * quarter * latent * 4 * cols,
        2 * quarter * latent * 2,
        in_specs=[smem] + [vmem] * 8,
        out_specs=[vmem] * 4,
    )
    row_parts = [terms[0]] + from_peers(terms, True)
    grid_grad = call(
        place_kernel,
        shape((grid_rows, LANES), BF16),
        (chan, *row_parts),
        0,
        4 * grid_rows * LANES,
        in_specs=[smem] + [vmem] * 4,
        out_specs=vmem,
    )
    node_terms = call(
        node_kernel,
        [shape((nodes, LANES), F32)] + [shape((nodes, LANES), BF16)] * 3,
        (chan, wanted, w_recv, *returned),
        2 * nodes * cols * (slot_count + 2 * latent),
        2 * nodes * latent,
        in_specs=[smem] + [vmem] * 9,
        out_specs=[vmem] * 4,
    )
    node_grad = node_terms[0]
    for part in from_peers(node_terms, True):
        node_grad = node_grad + part.astype(F32)
    return (grid_grad, node_grad.astype(BF16))


def solution(mesh):
    in_specs = (
        P("band", None),
        P("band", None),
        P("band", "mp"),
        P("band", "mp"),
        P("band"),
        P("band", None, None),
        P("band"),
        P("band"),
        P(None, "mp"),
        P(None, "mp"),
        P(None, "mp"),
        P("mp"),
        P("mp", None),
    )
    out_specs = (P("band", "mp"), P("band", "mp"))
    return jax.shard_map(
        per_device, mesh=mesh, in_specs=in_specs, out_specs=out_specs, check_vma=False
    )
```

```python
import jax
import jax.numpy as jnp
from jax import lax
from jax.experimental import pallas as pl
from jax.experimental.pallas import tpu as pltpu
from jax.sharding import PartitionSpec as P


F32 = jnp.float32
BF16 = jnp.bfloat16
I32 = jnp.int32
I16 = jnp.int16
LANES = 128
BLOCK = 256
WINDOW = 384
ROWS = 1024
OWN = 3
OTHERS = (2, 4, 1, 5, 0, 6)
ORDER = (OWN, *OTHERS)


def ring(shard, axis, by):
    devices = lax.axis_size(axis)
    return lax.ppermute(shard, axis, [(i, (i + by) % devices) for i in range(devices)])


def from_peers(shard, by_shift):
    return [ring(shard[s] if by_shift else shard, "mp", s) for s in (1, 2, 3)]


def dot(a, b):
    return jnp.dot(a, b, preferred_element_type=F32)


def dot_t(a, b):
    return lax.dot_general(a, b, (((1,), (1,)), ((), ())), preferred_element_type=F32)


def column(row):
    return jnp.transpose(jnp.broadcast_to(row, (LANES, row.shape[1])))


def one_hot(ids, width):
    short = ids.astype(I16)
    lane = lax.broadcasted_iota(I32, ids.shape, 1).astype(I16)
    one, zero = jnp.ones(ids.shape, BF16), jnp.zeros(ids.shape, BF16)
    return jnp.concatenate(
        [jnp.where(short == lane + jnp.int16(LANES * t), one, zero) for t in range(width // LANES)], axis=1
    )


def one_hot_t(row, height):
    shape = (height, row.shape[1])
    return (jnp.broadcast_to(row, shape) == lax.broadcasted_iota(I32, shape, 0)).astype(F32).astype(BF16)


def call(kernel, out_shape, args, flops, nbytes, mib, **kw):
    return pl.pallas_call(
        kernel,
        out_shape=out_shape,
        cost_estimate=pl.CostEstimate(flops=flops, bytes_accessed=nbytes, transcendentals=0),
        compiler_params=pltpu.CompilerParams(vmem_limit_bytes=mib * 2**20),
        **kw,
    )(*args)


def shape(dims, dtype):
    return jax.ShapeDtypeStruct(dims, dtype)


def pick_kernel(lat_ref, grad_ref, counts_ref, req_ref, *out_refs):
    nodes = lat_ref.shape[0]
    scaled = []
    for t in range(nodes // LANES):
        rows = pl.ds(LANES * t, LANES)
        count = column(counts_ref[t : t + 1, :]).astype(F32)
        scaled.append((grad_ref[rows, :].astype(F32) / count).astype(BF16))
    both = jnp.concatenate([lat_ref[...], jnp.concatenate(scaled, axis=0)], axis=1)
    for k, out_ref in enumerate(out_refs):
        ids = column(req_ref[k])
        out_ref[...] = dot(one_hot(ids, nodes), both).astype(BF16)


def join_kernel(*refs):
    out_ref = refs[-1]
    for n, ref in enumerate(refs[:-1]):
        out_ref[n * LANES : (n + 1) * LANES, :] = ref[...]


def pre_kernel(base_ref, lat_ref, edge_ref, send_ref, slot_ref, wsend_ref, wedge_ref, bias_ref, *refs):
    out_ref, slot_hot_ref, send_hot_ref, split_ref = refs
    cols = wsend_ref.shape[1]
    slot_count = slot_hot_ref.shape[1]
    lat_steps = lat_ref.shape[0] // ROWS
    steps = edge_ref.shape[0] // ROWS

    def at(step):
        return pl.ds(pl.multiple_of(step * ROWS, ROWS), ROWS)

    @pl.loop(0, lat_steps)
    def _(step):
        proj = dot(lat_ref[at(step), :], wsend_ref[...])
        upper = proj.astype(BF16)
        lower = (proj - upper.astype(F32)).astype(BF16)
        split_ref[at(step), :] = jnp.concatenate([upper, lower], axis=1)

    @pl.loop(0, steps)
    def _(step):
        for sub in range(ROWS // BLOCK):
            block = step * (ROWS // BLOCK) + sub
            rows = pl.ds(pl.multiple_of(block * BLOCK, BLOCK), BLOCK)
            base = pl.multiple_of(base_ref[block], LANES)
            send_row = send_ref[pl.ds(block, 1), :] - base
            slot_row = slot_ref[pl.ds(block, 1), :]
            send_hot = one_hot(column(send_row), WINDOW)
            picked = dot(send_hot, split_ref[pl.ds(base, WINDOW), :])
            value = picked[:, :cols] + picked[:, cols:] + dot(edge_ref[rows, :], wedge_ref[...])
            out_ref[rows, :] = value + bias_ref[...]
            send_hot_ref[rows, :] = send_hot
            slot_hot_ref[rows, :] = one_hot(column(slot_row), slot_count)


def main_kernel(base_ref, chan_ref, *refs):
    slots_in, recv_ref, wout_ref = refs[:4], refs[4], refs[5]
    pre_ref, slot_hot_ref, send_hot_ref = refs[6:9]
    sums, slots = refs[9:13], refs[13:20]
    table_ref, acc_ref, slot_acc_ref, grad_ref = refs[20:]
    cols = recv_ref.shape[1]
    steps = pre_ref.shape[0] // ROWS

    acc_ref[...] = jnp.zeros_like(acc_ref)
    slot_acc_ref[...] = jnp.zeros_like(slot_acc_ref)
    proj = back = None
    for s, ref in enumerate(slots_in):
        chan = pl.ds(pl.multiple_of(chan_ref[s], LANES), LANES)
        p = dot(ref[:, :LANES], recv_ref[chan, :])
        b = dot_t(ref[:, LANES:], wout_ref[:, chan])
        proj = p if proj is None else proj + p
        back = b if back is None else back + b
    both = jnp.concatenate([proj, back], axis=1).astype(BF16)
    for n, k in enumerate(ORDER):
        table_ref[k * LANES : (k + 1) * LANES, :] = both[n * LANES : (n + 1) * LANES, :]

    def at(start, size):
        return pl.ds(pl.multiple_of(start, size), size)

    def gradient(step):
        rows = at(step * ROWS, ROWS)
        got = dot(slot_hot_ref[rows, :], table_ref[...])
        pre = pre_ref[rows, :] + got[:, :cols]
        sig = jax.nn.sigmoid(pre)
        return jnp.transpose(got[:, cols:] * (sig * (1.0 + pre * (1.0 - sig)))).astype(BF16)

    def collect(step, grad):
        slot_acc_ref[...] += dot(grad, slot_hot_ref[at(step * ROWS, ROWS), :])
        for sub in range(ROWS // BLOCK):
            block = step * (ROWS // BLOCK) + sub
            base = pl.multiple_of(base_ref[block], LANES)
            part = grad[:, sub * BLOCK : (sub + 1) * BLOCK]
            acc_ref[:, pl.ds(base, WINDOW)] += dot(part, send_hot_ref[at(block * BLOCK, BLOCK), :])

    grad_ref[...] = gradient(0)

    @pl.loop(1, steps)
    def _(step):
        before = grad_ref[...]
        grad = gradient(step)
        collect(step - 1, before)
        grad_ref[...] = grad

    collect(steps - 1, grad_ref[...])
    quarter = sums[0].shape[0]
    for s, out_ref in enumerate(sums):
        first = pl.multiple_of(chan_ref[4 + s] // LANES * quarter, LANES)
        for n in range(quarter // LANES):
            part = acc_ref[:, pl.ds(pl.multiple_of(first + n * LANES, LANES), LANES)]
            out_ref[n * LANES : (n + 1) * LANES, :] = jnp.transpose(part).astype(BF16)
    for k, out_ref in enumerate(slots):
        out_ref[...] = jnp.transpose(slot_acc_ref[:, k * LANES : (k + 1) * LANES]).astype(BF16)


def back_kernel(chan_ref, *refs):
    parts, weights, outs = refs[:4], refs[4:8], refs[8:12]
    x = jnp.concatenate([r[...] for r in parts], axis=1)
    for s, out_ref in enumerate(outs):
        chan = pl.ds(pl.multiple_of(chan_ref[4 + s], LANES), LANES)
        w = jnp.concatenate([r[chan, :] for r in weights], axis=1)
        out_ref[...] = dot_t(x, w).astype(BF16)


def place_kernel(chan_ref, *refs):
    out_ref = refs[4]
    quarter = refs[0].shape[0]
    for s in range(4):
        first = pl.multiple_of(chan_ref[s] // LANES * quarter, LANES)
        out_ref[pl.ds(first, quarter), :] = refs[s][...]


def node_kernel(chan_ref, req_ref, recv_ref, *refs):
    returned, outs = refs[:7], refs[7:11]
    nodes = outs[0].shape[0]
    picks = jnp.concatenate([one_hot_t(req_ref[k], nodes) for k in range(len(returned))], axis=1)
    total = dot(picks, jnp.concatenate([ref[...] for ref in returned], axis=0))
    upper = total.astype(BF16)
    lower = (total - upper.astype(F32)).astype(BF16)
    for s, out_ref in enumerate(outs):
        w = recv_ref[pl.ds(pl.multiple_of(chan_ref[4 + s], LANES), LANES), :]
        out_ref[...] = (dot_t(upper, w) + dot_t(lower, w)).astype(out_ref.dtype)


def per_device(
    grid_latent,
    edge_latent,
    mesh_latent,
    mesh_grad,
    counts,
    request,
    edge_sender,
    edge_slot,
    w_send,
    w_recv,
    w_edge,
    edge_bias,
    w_out,
):
    span, capacity = request.shape[1:]
    nodes = mesh_latent.shape[0]
    grid_rows, latent = grid_latent.shape
    edges = edge_latent.shape[0]
    cols = w_send.shape[1]
    slot_count = span * capacity
    blocks = edges // BLOCK
    quarter = grid_rows // 4
    mine = lax.axis_index("mp")
    turns = jnp.arange(4, dtype=I32)
    chan = jnp.concatenate([(mine - turns) % 4, (mine + turns) % 4]).astype(I32) * LANES
    senders = edge_sender.reshape(blocks, BLOCK)
    slot_ids = edge_slot.reshape(blocks, BLOCK)
    base = jnp.minimum(senders[:, 0] // LANES * LANES, grid_rows - WINDOW)
    wanted = request.reshape(span, 1, capacity)

    smem = pl.BlockSpec(memory_space=pltpu.SMEM)
    vmem = pl.BlockSpec(memory_space=pltpu.VMEM)
    picked = call(
        pick_kernel,
        [shape((capacity, 2 * LANES), BF16)] * span,
        (mesh_latent, mesh_grad, counts.reshape(nodes // LANES, LANES), wanted),
        2 * slot_count * nodes * 2 * LANES,
        2 * (2 * nodes + 2 * slot_count) * LANES,
        60,
        in_specs=[vmem] * 4,
        out_specs=[vmem] * span,
    )
    slots_here = call(
        join_kernel,
        shape((slot_count, 2 * LANES), BF16),
        (picked[OWN], *[ring(picked[k], "band", OWN - k) for k in OTHERS]),
        0,
        8 * slot_count * LANES,
        4,
        in_specs=[vmem] * span,
        out_specs=vmem,
    )
    slots_all = [slots_here] + from_peers(slots_here, False)
    send_peers = from_peers(w_send, False)

    pre, *hots = call(
        pre_kernel,
        [shape((edges, cols), F32), shape((edges, slot_count), BF16), shape((edges, WINDOW), BF16)],
        (base, grid_latent, edge_latent, senders, slot_ids, w_send, w_edge, edge_bias.reshape(1, cols)),
        2 * edges * cols * (latent + 2 * WINDOW) + 2 * grid_rows * latent * cols,
        2 * (edges + grid_rows) * latent + 4 * edges * cols,
        6,
        in_specs=[smem] + [vmem] * 7,
        out_specs=[vmem] * 3,
        scratch_shapes=[pltpu.VMEM((grid_rows, 2 * cols), BF16)],
    )
    result = call(
        main_kernel,
        [shape((quarter, cols), BF16)] * 4 + [shape((capacity, cols), BF16)] * span,
        (base, chan, *slots_all, w_recv, w_out, pre, *hots),
        2 * edges * cols * (3 * slot_count + WINDOW),
        4 * edges * cols,
        8,
        in_specs=[smem, smem] + [vmem] * 9,
        out_specs=[vmem] * 11,
        scratch_shapes=[
            pltpu.VMEM((slot_count, 2 * cols), BF16),
            pltpu.VMEM((cols, grid_rows), F32),
            pltpu.VMEM((cols, slot_count), F32),
            pltpu.VMEM((cols, ROWS), BF16),
        ],
    )
    sums, slot_sums = result[:4], result[4:]

    back = {k: ring(slot_sums[k], "band", k - OWN) for k in OTHERS}
    back[OWN] = slot_sums[OWN]
    hidden_parts = [sums[0]] + from_peers(sums, True)
    node_terms = call(
        node_kernel,
        [shape((nodes, LANES), F32)] + [shape((nodes, LANES), BF16)] * 3,
        (chan, wanted, w_recv, *[back[k] for k in range(span)]),
        2 * nodes * cols * (slot_count + 2 * latent),
        2 * nodes * latent,
        8,
        in_specs=[smem] + [vmem] * 9,
        out_specs=[vmem] * 4,
    )
    terms = call(
        back_kernel,
        [shape((quarter, LANES), BF16)] * 4,
        (chan, *hidden_parts, w_send, *send_peers),
        2 * quarter * latent * 4 * cols,
        2 * quarter * latent * 2,
        8,
        in_specs=[smem] + [vmem] * 8,
        out_specs=[vmem] * 4,
    )
    row_parts = [terms[0]] + from_peers(terms, True)
    grid_grad = call(
        place_kernel,
        shape((grid_rows, LANES), BF16),
        (chan, *row_parts),
        0,
        4 * grid_rows * LANES,
        8,
        in_specs=[smem] + [vmem] * 4,
        out_specs=vmem,
    )
    node_grad = node_terms[0]
    for part in from_peers(node_terms, True):
        node_grad = node_grad + part.astype(F32)
    return (grid_grad, node_grad.astype(BF16))


def solution(mesh):
    in_specs = (
        P("band", None),
        P("band", None),
        P("band", "mp"),
        P("band", "mp"),
        P("band"),
        P("band", None, None),
        P("band"),
        P("band"),
        P(None, "mp"),
        P(None, "mp"),
        P(None, "mp"),
        P("mp"),
        P("mp", None),
    )
    out_specs = (P("band", "mp"), P("band", "mp"))

    return jax.shard_map(per_device, mesh=mesh, in_specs=in_specs, out_specs=out_specs, check_vma=False)
```

```python
import jax
import jax.numpy as jnp
from jax import lax
from jax.experimental import pallas as pl
from jax.experimental.pallas import tpu as pltpu
from jax.sharding import PartitionSpec as P


F32 = jnp.float32
BF16 = jnp.bfloat16
I32 = jnp.int32
I16 = jnp.int16
LANES = 128
BLOCK = 256
WINDOW = 384
ROWS = 1024
OWN = 3
OTHERS = (2, 1, 0, 4, 5, 6)
ORDER = (OWN, *OTHERS)


def ring(shard, axis, by):
    devices = lax.axis_size(axis)
    return lax.ppermute(shard, axis, [(i, (i + by) % devices) for i in range(devices)])


def from_peers(shard, by_shift):
    return [ring(shard[s] if by_shift else shard, "mp", s) for s in (1, 2, 3)]


def dot(a, b):
    return jnp.dot(a, b, preferred_element_type=F32)


def dot_t(a, b):
    return lax.dot_general(a, b, (((1,), (1,)), ((), ())), preferred_element_type=F32)


def column(row):
    return jnp.transpose(jnp.broadcast_to(row, (LANES, row.shape[1])))


def one_hot(ids, width):
    short = ids.astype(I16)
    lane = lax.broadcasted_iota(I32, ids.shape, 1).astype(I16)
    one, zero = jnp.ones(ids.shape, BF16), jnp.zeros(ids.shape, BF16)
    return jnp.concatenate(
        [jnp.where(short == lane + jnp.int16(LANES * t), one, zero) for t in range(width // LANES)], axis=1
    )


def one_hot_t(row, height):
    shape = (height, row.shape[1])
    return (jnp.broadcast_to(row, shape) == lax.broadcasted_iota(I32, shape, 0)).astype(F32).astype(BF16)


def call(kernel, out_shape, args, flops, nbytes, mib, **kw):
    return pl.pallas_call(
        kernel,
        out_shape=out_shape,
        cost_estimate=pl.CostEstimate(flops=flops, bytes_accessed=nbytes, transcendentals=0),
        compiler_params=pltpu.CompilerParams(vmem_limit_bytes=mib * 2**20),
        **kw,
    )(*args)


def shape(dims, dtype):
    return jax.ShapeDtypeStruct(dims, dtype)


def pick_kernel(lat_ref, grad_ref, counts_ref, req_ref, *out_refs):
    nodes = lat_ref.shape[0]
    scaled = []
    for t in range(nodes // LANES):
        rows = pl.ds(LANES * t, LANES)
        count = column(counts_ref[t : t + 1, :]).astype(F32)
        scaled.append((grad_ref[rows, :].astype(F32) / count).astype(BF16))
    both = jnp.concatenate([lat_ref[...], jnp.concatenate(scaled, axis=0)], axis=1)
    for k, out_ref in enumerate(out_refs):
        ids = column(req_ref[k])
        out_ref[...] = dot(one_hot(ids, nodes), both).astype(BF16)


def join_kernel(*refs):
    out_ref = refs[-1]
    for n, ref in enumerate(refs[:-1]):
        out_ref[n * LANES : (n + 1) * LANES, :] = ref[...]


def pre_kernel(base_ref, lat_ref, edge_ref, send_ref, slot_ref, wsend_ref, wedge_ref, bias_ref, *refs):
    out_ref, slot_hot_ref, send_hot_ref, split_ref = refs
    cols = wsend_ref.shape[1]
    slot_count = slot_hot_ref.shape[1]
    lat_steps = lat_ref.shape[0] // ROWS
    steps = edge_ref.shape[0] // ROWS

    def at(step):
        return pl.ds(pl.multiple_of(step * ROWS, ROWS), ROWS)

    @pl.loop(0, lat_steps)
    def _(step):
        proj = dot(lat_ref[at(step), :], wsend_ref[...])
        upper = proj.astype(BF16)
        lower = (proj - upper.astype(F32)).astype(BF16)
        split_ref[at(step), :] = jnp.concatenate([upper, lower], axis=1)

    @pl.loop(0, steps)
    def _(step):
        for sub in range(ROWS // BLOCK):
            block = step * (ROWS // BLOCK) + sub
            rows = pl.ds(pl.multiple_of(block * BLOCK, BLOCK), BLOCK)
            base = pl.multiple_of(base_ref[block], LANES)
            send_row = send_ref[pl.ds(block, 1), :] - base
            slot_row = slot_ref[pl.ds(block, 1), :]
            send_hot = one_hot(column(send_row), WINDOW)
            picked = dot(send_hot, split_ref[pl.ds(base, WINDOW), :])
            value = picked[:, :cols] + picked[:, cols:] + dot(edge_ref[rows, :], wedge_ref[...])
            out_ref[rows, :] = value + bias_ref[...]
            send_hot_ref[rows, :] = send_hot
            slot_hot_ref[rows, :] = one_hot(column(slot_row), slot_count)


def main_kernel(base_ref, chan_ref, *refs):
    slots_in, recv_ref, wout_ref = refs[:4], refs[4], refs[5]
    pre_ref, slot_hot_ref, send_hot_ref = refs[6:9]
    sums, slots = refs[9:13], refs[13:20]
    table_ref, acc_ref, slot_acc_ref, grad_ref = refs[20:]
    cols = recv_ref.shape[1]
    steps = pre_ref.shape[0] // ROWS

    acc_ref[...] = jnp.zeros_like(acc_ref)
    slot_acc_ref[...] = jnp.zeros_like(slot_acc_ref)
    proj = back = None
    for s, ref in enumerate(slots_in):
        chan = pl.ds(pl.multiple_of(chan_ref[s], LANES), LANES)
        p = dot(ref[:, :LANES], recv_ref[chan, :])
        b = dot_t(ref[:, LANES:], wout_ref[:, chan])
        proj = p if proj is None else proj + p
        back = b if back is None else back + b
    both = jnp.concatenate([proj, back], axis=1).astype(BF16)
    for n, k in enumerate(ORDER):
        table_ref[k * LANES : (k + 1) * LANES, :] = both[n * LANES : (n + 1) * LANES, :]

    def at(start, size):
        return pl.ds(pl.multiple_of(start, size), size)

    def gradient(step):
        rows = at(step * ROWS, ROWS)
        got = dot(slot_hot_ref[rows, :], table_ref[...])
        pre = pre_ref[rows, :] + got[:, :cols]
        sig = jax.nn.sigmoid(pre)
        return jnp.transpose(got[:, cols:] * (sig * (1.0 + pre * (1.0 - sig)))).astype(BF16)

    def collect(step, grad):
        slot_acc_ref[...] += dot(grad, slot_hot_ref[at(step * ROWS, ROWS), :])
        for sub in range(ROWS // BLOCK):
            block = step * (ROWS // BLOCK) + sub
            base = pl.multiple_of(base_ref[block], LANES)
            part = grad[:, sub * BLOCK : (sub + 1) * BLOCK]
            acc_ref[:, pl.ds(base, WINDOW)] += dot(part, send_hot_ref[at(block * BLOCK, BLOCK), :])

    grad_ref[...] = gradient(0)

    @pl.loop(1, steps)
    def _(step):
        before = grad_ref[...]
        grad = gradient(step)
        collect(step - 1, before)
        grad_ref[...] = grad

    collect(steps - 1, grad_ref[...])
    quarter = sums[0].shape[0]
    for s, out_ref in enumerate(sums):
        first = pl.multiple_of(chan_ref[4 + s] // LANES * quarter, LANES)
        for n in range(quarter // LANES):
            part = acc_ref[:, pl.ds(pl.multiple_of(first + n * LANES, LANES), LANES)]
            out_ref[n * LANES : (n + 1) * LANES, :] = jnp.transpose(part).astype(BF16)
    for k, out_ref in enumerate(slots):
        out_ref[...] = jnp.transpose(slot_acc_ref[:, k * LANES : (k + 1) * LANES]).astype(BF16)


def back_kernel(chan_ref, *refs):
    parts, weights, outs = refs[:4], refs[4:8], refs[8:12]
    x = jnp.concatenate([r[...] for r in parts], axis=1)
    for s, out_ref in enumerate(outs):
        chan = pl.ds(pl.multiple_of(chan_ref[4 + s], LANES), LANES)
        w = jnp.concatenate([r[chan, :] for r in weights], axis=1)
        out_ref[...] = dot_t(x, w).astype(BF16)


def place_kernel(chan_ref, *refs):
    out_ref = refs[4]
    quarter = refs[0].shape[0]
    for s in range(4):
        first = pl.multiple_of(chan_ref[s] // LANES * quarter, LANES)
        out_ref[pl.ds(first, quarter), :] = refs[s][...]


def node_kernel(chan_ref, req_ref, recv_ref, *refs):
    returned, outs = refs[:7], refs[7:11]
    nodes = outs[0].shape[0]
    picks = jnp.concatenate([one_hot_t(req_ref[k], nodes) for k in range(len(returned))], axis=1)
    total = dot(picks, jnp.concatenate([ref[...] for ref in returned], axis=0))
    upper = total.astype(BF16)
    lower = (total - upper.astype(F32)).astype(BF16)
    for s, out_ref in enumerate(outs):
        w = recv_ref[pl.ds(pl.multiple_of(chan_ref[4 + s], LANES), LANES), :]
        out_ref[...] = (dot_t(upper, w) + dot_t(lower, w)).astype(out_ref.dtype)


def per_device(
    grid_latent,
    edge_latent,
    mesh_latent,
    mesh_grad,
    counts,
    request,
    edge_sender,
    edge_slot,
    w_send,
    w_recv,
    w_edge,
    edge_bias,
    w_out,
):
    span, capacity = request.shape[1:]
    nodes = mesh_latent.shape[0]
    grid_rows, latent = grid_latent.shape
    edges = edge_latent.shape[0]
    cols = w_send.shape[1]
    slot_count = span * capacity
    blocks = edges // BLOCK
    quarter = grid_rows // 4
    mine = lax.axis_index("mp")
    turns = jnp.arange(4, dtype=I32)
    chan = jnp.concatenate([(mine - turns) % 4, (mine + turns) % 4]).astype(I32) * LANES
    senders = edge_sender.reshape(blocks, BLOCK)
    slot_ids = edge_slot.reshape(blocks, BLOCK)
    base = jnp.minimum(senders[:, 0] // LANES * LANES, grid_rows - WINDOW)
    wanted = request.reshape(span, 1, capacity)

    smem = pl.BlockSpec(memory_space=pltpu.SMEM)
    vmem = pl.BlockSpec(memory_space=pltpu.VMEM)
    picked = call(
        pick_kernel,
        [shape((capacity, 2 * LANES), BF16)] * span,
        (mesh_latent, mesh_grad, counts.reshape(nodes // LANES, LANES), wanted),
        2 * slot_count * nodes * 2 * LANES,
        2 * (2 * nodes + 2 * slot_count) * LANES,
        60,
        in_specs=[vmem] * 4,
        out_specs=[vmem] * span,
    )
    arrived = [ring(picked[k], "band", OWN - k) for k in OTHERS]
    slots_here = call(
        join_kernel,
        shape((slot_count, 2 * LANES), BF16),
        (picked[OWN], *arrived),
        0,
        8 * slot_count * LANES,
        4,
        in_specs=[vmem] * span,
        out_specs=vmem,
    )
    slots_all = [slots_here] + from_peers(slots_here, False)
    send_peers = from_peers(w_send, False)

    pre, *hots = call(
        pre_kernel,
        [shape((edges, cols), F32), shape((edges, slot_count), BF16), shape((edges, WINDOW), BF16)],
        (base, grid_latent, edge_latent, senders, slot_ids, w_send, w_edge, edge_bias.reshape(1, cols)),
        2 * edges * cols * (latent + 2 * WINDOW) + 2 * grid_rows * latent * cols,
        2 * (edges + grid_rows) * latent + 4 * edges * cols,
        6,
        in_specs=[smem] + [vmem] * 7,
        out_specs=[vmem] * 3,
        scratch_shapes=[pltpu.VMEM((grid_rows, 2 * cols), BF16)],
    )
    result = call(
        main_kernel,
        [shape((quarter, cols), BF16)] * 4 + [shape((capacity, cols), BF16)] * span,
        (base, chan, *slots_all, w_recv, w_out, pre, *hots),
        2 * edges * cols * (3 * slot_count + WINDOW),
        4 * edges * cols,
        8,
        in_specs=[smem, smem] + [vmem] * 9,
        out_specs=[vmem] * 11,
        scratch_shapes=[
            pltpu.VMEM((slot_count, 2 * cols), BF16),
            pltpu.VMEM((cols, grid_rows), F32),
            pltpu.VMEM((cols, slot_count), F32),
            pltpu.VMEM((cols, ROWS), BF16),
        ],
    )
    sums, slot_sums = result[:4], result[4:]

    hidden_parts = [sums[0]] + from_peers(sums, True)
    back = {k: ring(slot_sums[k], "band", k - OWN) for k in OTHERS}
    back[OWN] = slot_sums[OWN]
    node_terms = call(
        node_kernel,
        [shape((nodes, LANES), F32)] + [shape((nodes, LANES), BF16)] * 3,
        (chan, wanted, w_recv, *[back[k] for k in range(span)]),
        2 * nodes * cols * (slot_count + 2 * latent),
        2 * nodes * latent,
        8,
        in_specs=[smem] + [vmem] * 9,
        out_specs=[vmem] * 4,
    )
    terms = call(
        back_kernel,
        [shape((quarter, LANES), BF16)] * 4,
        (chan, *hidden_parts, w_send, *send_peers),
        2 * quarter * latent * 4 * cols,
        2 * quarter * latent * 2,
        8,
        in_specs=[smem] + [vmem] * 8,
        out_specs=[vmem] * 4,
    )
    row_parts = [terms[0]] + from_peers(terms, True)
    grid_grad = call(
        place_kernel,
        shape((grid_rows, LANES), BF16),
        (chan, *row_parts),
        0,
        4 * grid_rows * LANES,
        8,
        in_specs=[smem] + [vmem] * 4,
        out_specs=vmem,
    )
    node_parts = from_peers(node_terms, True)
    node_grad = node_terms[0]
    for part in node_parts:
        node_grad = node_grad + part.astype(F32)
    return (grid_grad, node_grad.astype(BF16))


def solution(mesh):
    in_specs = (
        P("band", None),
        P("band", None),
        P("band", "mp"),
        P("band", "mp"),
        P("band"),
        P("band", None, None),
        P("band"),
        P("band"),
        P(None, "mp"),
        P(None, "mp"),
        P(None, "mp"),
        P("mp"),
        P("mp", None),
    )
    out_specs = (P("band", "mp"), P("band", "mp"))

    return jax.shard_map(per_device, mesh=mesh, in_specs=in_specs, out_specs=out_specs, check_vma=False)
```
